128 devices in a mesh: row: 16 (over x_hi, z, core), col: 8 (over x_lo, y).
Axes of the slice: x: 4 (x_hi: 2, x_lo: 2; x = x_hi * 2 + x_lo), y: 4, z: 4, core: 2. Of those that a mesh axis runs over, the one named last changes fastest.
Arguments:
- local_inverse: float32 [1024, 512, 512], P(('row', 'col')), may hold values from -1 to 3.5, as said below
- coupling: float32 [1024, 512, 1024], P(('row', 'col')), may hold values from -0.03125 to 0.03125
- local_rhs: float32 [1024, 512], P(('row', 'col')), may hold values from -6 to 6
- members: int32 [1024, 8], P(('row', 'col')), may hold values from 0 to 15, all different within a row
- shared_matrix: float32 [2048, 2048], P('row', 'col'), may hold values from -2 to 66, as said below
- shared_rhs: float32 [2048], P('row'), may hold values from -6 to 6
- prior_solution: float32 [2048], P('row'), may hold values from -6 to 6
- preconditioner: float32 [2048], P('row'), may hold values from 0.008 to 0.02
Outputs:
- reduced_matrix: float32 [2048, 2048], P('row', 'col')
- reduced_rhs: float32 [2048], P('row')
- solution: float32 [2048], P('row')
The draws below stay inside these ranges and needn't reach their ends.
Inputs may be any that keep to these rules, and one draw needn't show every extreme that they name: `members`: each week names 8 different station blocks. `local_inverse`: symmetric for every week. `shared_matrix`: symmetric.
All inputs are finite; a program needn't handle non-finite values.
Results may differ from the reference program's by a relative error of at most 0.00016.
Values sent between devices are 32-bit elements; how exact they have to be, the bound alone decides.
No kernel may reach another device: no remote copies, remote signals or barrier semaphores. Data moves between devices by JAX's collectives and lax.ppermute only.
A program may use at most 256 MiB of HBM per device.

```python
import math
import jax
import jax.numpy as jnp
from jax import lax

LOCAL = 512
BLOCK = 128
BLOCKS = 16
TOUCHED = 8
ITERS = 2
WEEKS = 1024
SHARED = 2048


def draw_local_inverse(key, part):
    first, second = jax.random.split(jax.random.fold_in(key, 11))
    diagonal = jax.random.uniform(first, (WEEKS, LOCAL), jnp.float32, 1.0, 2.0)
    noise = jax.random.truncated_normal(second, -4.0, 4.0, (WEEKS, LOCAL, LOCAL), jnp.float32)
    spread = 0.4 / math.sqrt(2.0 * LOCAL)
    symmetric = (noise + jnp.swapaxes(noise, 1, 2)) * spread
    return symmetric + diagonal[:, :, None] * jnp.eye(LOCAL, dtype=jnp.float32)[None, :, :]


def draw_shared_matrix(key, part):
    first, second = jax.random.split(jax.random.fold_in(key, 23))
    diagonal = jax.random.uniform(first, (SHARED,), jnp.float32, 45.0, 60.0)
    noise = jax.random.truncated_normal(second, -4.0, 4.0, (SHARED, SHARED), jnp.float32)
    spread = 2.2 / math.sqrt(2.0 * SHARED)
    symmetric = (noise + noise.T) * spread
    return symmetric + jnp.diag(diagonal)


def levels(stream_key, shape, cuts, least, largest):
    level, own = 1.0, jax.random.fold_in(stream_key, 6)
    for dim, shards_of in cuts:
        heights = jnp.exp(jax.random.uniform(jax.random.fold_in(own, dim), (shards_of,), jnp.float32, least / len(cuts), largest / len(cuts)))
        level = level * jnp.repeat(heights, shape[dim] // shards_of).reshape([-1 if axis == dim else 1 for axis in range(len(shape))])
    return level


def different_ones(stream_key, rows, amount, top, lift):
    sequence = jax.random.permutation(jax.random.fold_in(stream_key, 1), amount)
    pull = sequence
    for power in range(3):
        pull = pull * pull // amount
    pull = pull * lift // amount
    tickets = jax.random.randint(jax.random.fold_in(stream_key, 2), (rows, amount), 0, 4096) + pull
    sure = jax.random.permutation(jax.random.fold_in(stream_key, 3), rows)[jnp.arange(amount) % rows]
    tickets = jnp.where(jnp.arange(rows)[:, None] == sure[None, :], 1 << 14, tickets)
    priority = tickets * amount + jnp.arange(amount)
    return lax.top_k(priority.astype(jnp.int32), top)[1].astype(jnp.int32)


def centred(stream_key, shape, scale, most, shards=(), held_as=jnp.bfloat16):
    entries = scale * jax.random.normal(stream_key, shape, jnp.float32)
    if shards:
        entries = entries * levels(stream_key, shape, shards, -0.22, 0.18)
    return jnp.clip(entries, -most, most).astype(held_as)


def setup_inputs(seed: int = 0) -> dict:
    keys = jax.random.split(jax.random.key(seed), 9)
    return {
        "local_inverse": draw_local_inverse(jax.random.fold_in(keys[8], 71), 0),
        "coupling": centred(keys[1], (WEEKS, LOCAL, TOUCHED * BLOCK), (LOCAL * WEEKS // 16) ** -0.5, 0.03125, ((0, 128),), jnp.float32),
        "local_rhs": centred(keys[2], (WEEKS, LOCAL), 1.0, 6.0, ((0, 128),), jnp.float32),
        "members": different_ones(keys[3], WEEKS, BLOCKS, TOUCHED, 4096),
        "shared_matrix": draw_shared_matrix(jax.random.fold_in(keys[8], 71), 0),
        "shared_rhs": centred(keys[5], (SHARED,), 1.0, 6.0, ((0, 16),), jnp.float32),
        "prior_solution": centred(keys[6], (SHARED,), 1.0, 6.0, ((0, 16),), jnp.float32),
        "preconditioner": jnp.clip(jnp.exp(math.log(0.02) - 0.91629066 * jax.random.uniform(keys[7], (SHARED,), jnp.float32) ** levels(keys[7], (SHARED,), ((0, 16),), -0.2, 0.2)), 0.008, 0.02),
    }


def eliminate(accumulated, items):
    grid_sum, rhs_sum = accumulated
    inverse, coupling_week, rhs_week, blocks = items
    mapped = jnp.dot(inverse, coupling_week, precision=lax.Precision.HIGHEST, preferred_element_type=jnp.float32)
    contribution = jnp.dot(coupling_week.T, mapped, precision=lax.Precision.HIGHEST, preferred_element_type=jnp.float32)
    pushed = jnp.dot(rhs_week, mapped, precision=lax.Precision.HIGHEST, preferred_element_type=jnp.float32)
    tile_grid = contribution.reshape(TOUCHED, BLOCK, TOUCHED, BLOCK).transpose(0, 2, 1, 3)
    grid_sum = grid_sum.at[blocks[:, None], blocks[None, :]].add(tile_grid)
    rhs_sum = rhs_sum.at[blocks].add(pushed.reshape(TOUCHED, BLOCK))
    return (grid_sum, rhs_sum), None


def reference(local_inverse, coupling, local_rhs, members, shared_matrix, shared_rhs, prior_solution, preconditioner):
    start_grid = jnp.zeros((BLOCKS, BLOCKS, BLOCK, BLOCK), jnp.float32)
    start_rhs = jnp.zeros((BLOCKS, BLOCK), jnp.float32)
    (grid_sum, rhs_sum), unused = lax.scan(eliminate, (start_grid, start_rhs), (local_inverse, coupling, local_rhs, members.astype(jnp.int32)))
    eliminated = grid_sum.transpose(0, 2, 1, 3).reshape(SHARED, SHARED)
    reduced_matrix = shared_matrix - eliminated
    reduced_rhs = shared_rhs - rhs_sum.reshape(SHARED)
    solution = prior_solution
    for iteration in range(ITERS):
        product = jnp.dot(reduced_matrix, solution, precision=lax.Precision.HIGHEST, preferred_element_type=jnp.float32)
        solution = solution + preconditioner * (reduced_rhs - product)
    return (reduced_matrix, reduced_rhs, solution)
```

```python
import functools

import jax
import jax.numpy as jnp
from jax import lax
from jax.experimental import pallas as pl
from jax.experimental.pallas import tpu as pltpu
from jax.sharding import Mesh
from jax.sharding import PartitionSpec as P

BLOCK = 128
BLOCKS = 16
TOUCHED = 8
PAIRS = TOUCHED // 2
SUPERS = BLOCKS // 2
CHIPS = 64
EXTRA = 16
TAIL = 8
CHUNKS = ((0, 64), (64, 64))

AXES = ("x_hi", "z", "core", "x_lo", "y")
CHIP_AXES = ("x_hi", "z", "x_lo", "y")
COL = ("x_lo", "y")
F32 = jnp.float32
BF16 = jnp.bfloat16


def halves(values):
    high = values.astype(BF16)
    return high, (values - high.astype(F32)).astype(BF16)


def mul(left, right):
    return lax.dot_general(left, right, (((1,), (0,)), ((), ())), preferred_element_type=F32)


def mul_nt(left, right):
    return lax.dot_general(left, right, (((1,), (1,)), ((), ())), preferred_element_type=F32)


def place_of(low, high, core):
    low_super, low_odd = low // 2, low % 2
    high_super, high_odd = high // 2, high % 2
    same = low_odd == high_odd
    upper = jnp.logical_or(same, low_super == high_super)
    odd = jnp.where(low_super == high_super, 1, jnp.where(same, low_odd, high_odd))
    row = jnp.where(upper, low_super, high_super)
    column = jnp.where(upper, high_super, low_super)
    return (odd ^ core) * CHIPS + row * SUPERS + column


def eliminate_kernel(first, rows, last, *refs):
    members, place = refs[:2]
    refs = refs[2:]
    if last:
        inverse, coupling, rhs, prior, base, diag_in, keep, send = refs[:8]
        scratch = refs[8:]
        packed, ch, cl, ah, al, lh, ll, mh, ml, diag, ordered, sems, vec = scratch
    else:
        inverse, coupling, diag_in, keep, send, diag_out = refs[:6]
        scratch = refs[6:]
        packed, ch, cl, ah, al, lh, ll, mh, ml, diag, ordered, sems = scratch
    week = pl.program_id(0)
    core = place[0]
    extra = EXTRA if last else 0

    @pl.when(week == 0)
    def _():
        packed[...] = jnp.zeros_like(packed)
        diag[...] = diag_in[...]
        if last:
            vec[...] = jnp.zeros_like(vec)

    blocks = [members[week, slot] for slot in range(TOUCHED)]
    ranks = []
    for slot in range(TOUCHED):
        rank = jnp.int32(0)
        for other in range(TOUCHED):
            if other != slot:
                rank = rank + (blocks[other] < blocks[slot]).astype(jnp.int32)
        ordered[rank] = blocks[slot]
        ranks.append(rank)
    for slot in range(TOUCHED):
        tile = coupling[0, :, slot * BLOCK : (slot + 1) * BLOCK]
        high, low = halves(tile)
        at = pl.ds(pl.multiple_of(ranks[slot] * BLOCK, BLOCK), BLOCK)
        ch[:, at] = high
        cl[:, at] = low
        turned_high, turned_low = halves(tile.T[first : first + rows])
        at = pl.ds(pl.multiple_of(extra + ranks[slot] * rows, 16), rows)
        lh[at, :] = turned_high
        ll[at, :] = turned_low
    high, low = halves(inverse[0])
    ah[...] = high
    al[...] = low
    ordered_blocks = [ordered[slot] for slot in range(TOUCHED)]
    if last:
        known = jnp.concatenate([prior[block] for block in ordered_blocks], axis=1)
        known = jnp.broadcast_to(known, (EXTRA, TOUCHED * BLOCK))
        kh, kl = halves(known)
        image = mul_nt(kh, ch[...]) + mul_nt(kl, ch[...]) + mul_nt(kh, cl[...])
        week_rhs = rhs[0]
        index = lax.broadcasted_iota(jnp.int32, image.shape, 0)
        lead = jnp.where(
            index == 0, week_rhs, jnp.where(index == 1, image - week_rhs, 0.0)
        )
        lead_high, lead_low = halves(lead)
        lh[:EXTRA, :] = lead_high
        ll[:EXTRA, :] = lead_low
    mapped = mul(lh[...], ah[...]) + mul(ll[...], ah[...]) + mul(lh[...], al[...])
    high, low = halves(mapped)
    mh[...] = high
    ml[...] = low
    row = first + lax.broadcasted_iota(jnp.int32, (rows, BLOCK), 0)
    column = lax.broadcasted_iota(jnp.int32, (rows, BLOCK), 1)
    for pair in range(PAIRS):
        count = extra + (2 * pair + 2) * rows
        at = slice(pair * 2 * BLOCK, (pair + 1) * 2 * BLOCK)
        c_high, c_low = ch[:, at], cl[:, at]
        sums = mul(mh[:count], c_high) + mul(ml[:count], c_high) + mul(mh[:count], c_low)
        for right in range(2):
            b = 2 * pair + right
            block = ordered_blocks[b]
            if last:
                vec[block, 0:8, :] += sums[:8, right * BLOCK : (right + 1) * BLOCK]
            for a in range(b + 1):
                tile = sums[
                    extra + a * rows : extra + (a + 1) * rows,
                    right * BLOCK : (right + 1) * BLOCK,
                ]
                if a == b:
                    odd = block % 2
                    own = (core * CHIPS) + (block // 2) * (SUPERS + 1)
                    upper = (row <= column).astype(jnp.int32)
                    packed[own, :rows, :] += jnp.where(upper != odd, tile, 0.0)
                    line = jnp.sum(
                        jnp.where(row == column, tile, 0.0), axis=0, keepdims=True
                    ) * odd.astype(F32)
                    diag[block // 2, 0:1, :] += line
                else:
                    own = place_of(ordered_blocks[a], block, core)
                    packed[own, :rows, :] += tile

    @pl.when(week == pl.num_programs(0) - 1)
    def _():
        if last:
            vec[place[1], 1:2, :] += base[...]
            for odd in range(2):
                for chip_row in range(SUPERS):
                    own = vec[2 * chip_row + odd, 0:2, :]
                    for col in range(SUPERS):
                        at = (odd ^ core) * CHIPS + chip_row * SUPERS + col
                        packed[at, rows : rows + 2, :] = own
                        packed[at, rows + 2 : rows + 3, :] = vec[2 * col, 1:2, :]
                        packed[at, rows + 3 : rows + 4, :] = vec[2 * col + 1, 1:2, :]
                        if odd == 0 and chip_row == col:
                            packed[at, rows + 4 : rows + 5, :] = diag[col, 0:1, :]
        else:
            diag_out[...] = diag[...]
        first_copy = pltpu.make_async_copy(packed.at[pl.ds(0, CHIPS)], keep, sems.at[0])
        second_copy = pltpu.make_async_copy(packed.at[pl.ds(CHIPS, CHIPS)], send, sems.at[1])
        second_copy.start()
        first_copy.start()
        second_copy.wait()
        first_copy.wait()


def eliminate(first, rows, last, members, place, inverse, coupling, diag, rhs, prior, base):
    weeks, size, width = coupling.shape
    extra, tail = (EXTRA, TAIL) if last else (0, 0)
    count = extra + TOUCHED * rows
    piece = jax.ShapeDtypeStruct((CHIPS, rows + tail, BLOCK), F32)
    diag_shape = (SUPERS, 8, BLOCK)
    whole = lambda *shape: pl.BlockSpec(shape, lambda w, *_: (0,) * len(shape))
    in_specs = [
        pl.BlockSpec((1, size, size), lambda w, *_: (w, 0, 0)),
        pl.BlockSpec((1, size, width), lambda w, *_: (w, 0, 0)),
    ]
    args = [inverse, coupling]
    if last:
        in_specs += [
            pl.BlockSpec((1, 1, size), lambda w, *_: (w, 0, 0)),
            whole(BLOCKS, 1, BLOCK),
            whole(1, BLOCK),
        ]
        args += [rhs, prior, base]
    in_specs.append(whole(*diag_shape))
    args.append(diag)
    out_shape = [piece, piece]
    out_specs = [pl.BlockSpec(memory_space=pl.ANY)] * 2
    if not last:
        out_shape.append(jax.ShapeDtypeStruct(diag_shape, F32))
        out_specs.append(whole(*diag_shape))
    scratch = [
        pltpu.VMEM((2 * CHIPS, rows + tail, BLOCK), F32),
        pltpu.VMEM((size, width), BF16),
        pltpu.VMEM((size, width), BF16),
        pltpu.VMEM((size, size), BF16),
        pltpu.VMEM((size, size), BF16),
        pltpu.VMEM((count, size), BF16),
        pltpu.VMEM((count, size), BF16),
        pltpu.VMEM((count, size), BF16),
        pltpu.VMEM((count, size), BF16),
        pltpu.VMEM(diag_shape, F32),
        pltpu.SMEM((TOUCHED,), jnp.int32),
        pltpu.SemaphoreType.DMA((2,)),
    ]
    if last:
        scratch.append(pltpu.VMEM((BLOCKS, 8, BLOCK), F32))
    return pl.pallas_call(
        functools.partial(eliminate_kernel, first, rows, last),
        out_shape=out_shape,
        grid_spec=pltpu.PrefetchScalarGridSpec(
            num_scalar_prefetch=2,
            grid=(weeks,),
            in_specs=in_specs,
            out_specs=out_specs,
            scratch_shapes=scratch,
        ),
        compiler_params=pltpu.CompilerParams(
            dimension_semantics=("arbitrary",), vmem_limit_bytes=56 * 1024 * 1024
        ),
        cost_estimate=pl.CostEstimate(
            flops=weeks * 2 * 3 * rows * 8 * size * (size + 640),
            bytes_accessed=weeks * size * (size + width) * 4,
            transcendentals=0,
        ),
        name=f"eliminate_{first}",
    )(members, place, *args)


def tile_kernel(place, own, other, shared, shared_rhs, prior, scale, matrix, rhs, product, known):
    mine, col = place[1], place[2]
    odd = mine % 2
    half = mine // 2
    upper, lower, level = half < col, half > col, half == col
    first, second = own[:BLOCK, :], other[:BLOCK, :]
    first_turned, second_turned = first.T, second.T
    row = lax.broadcasted_iota(jnp.int32, (BLOCK, BLOCK), 0)
    column = lax.broadcasted_iota(jnp.int32, (BLOCK, BLOCK), 1)
    even_tile = jnp.where(row <= column, first, first_turned)
    odd_tile = jnp.where(
        row > column,
        second,
        jnp.where(row == column, other[BLOCK + 4 : BLOCK + 5, :], second_turned),
    )
    level_even = jnp.logical_and(level, odd == 0)
    level_odd = jnp.logical_and(level, odd == 1)
    turn = jnp.logical_or(lower, level_odd)
    own_tile = jnp.where(level_even, even_tile, jnp.where(turn, first_turned, first))
    other_tile = jnp.where(level_odd, odd_tile, jnp.where(lower, second_turned, second))
    own_left = jnp.logical_or(
        level, jnp.logical_or(jnp.logical_and(upper, odd == 0), jnp.logical_and(lower, odd == 1))
    )
    left = shared[:, :BLOCK] - jnp.where(own_left, own_tile, other_tile)
    right = shared[:, BLOCK:] - jnp.where(own_left, other_tile, own_tile)
    matrix[:, :BLOCK] = left
    matrix[:, BLOCK:] = right
    rhs[...] = shared_rhs[...] - own[BLOCK : BLOCK + 1, :]
    known[...] = prior[mine] + scale[mine] * own[BLOCK + 1 : BLOCK + 2, :]
    left_known = prior[2 * col] + scale[2 * col] * own[BLOCK + 2 : BLOCK + 3, :]
    right_known = prior[2 * col + 1] + scale[2 * col + 1] * own[BLOCK + 3 : BLOCK + 4, :]
    dims = (((1,), (1,)), ((), ()))
    times = functools.partial(
        lax.dot_general,
        dimension_numbers=dims,
        precision=lax.Precision.HIGHEST,
        preferred_element_type=F32,
    )
    left_known = jnp.broadcast_to(left_known, (8, BLOCK))
    right_known = jnp.broadcast_to(right_known, (8, BLOCK))
    product[...] = times(left_known, left) + times(right_known, right)


def own_tile(place, own, other, shared, shared_rhs, prior, scale):
    vmem = pl.BlockSpec(memory_space=pltpu.VMEM)
    line = jax.ShapeDtypeStruct((1, BLOCK), F32)
    return pl.pallas_call(
        tile_kernel,
        out_shape=[
            jax.ShapeDtypeStruct(shared.shape, F32),
            line,
            jax.ShapeDtypeStruct((8, BLOCK), F32),
            line,
        ],
        in_specs=[pl.BlockSpec(memory_space=pltpu.SMEM)] + [vmem] * 6,
        out_specs=[vmem] * 4,
        name="own_tile",
    )(place, own, other, shared, shared_rhs, prior, scale)


def gathered(values):
    for axis in ("core", "z", "x_hi"):
        count = lax.axis_size(axis)
        here = lax.axis_index(axis)
        whole = jnp.zeros((count, *values.shape), F32)
        whole = lax.dynamic_update_slice_in_dim(whole, values[None], here, 0)
        for shift in range(1, count):
            pairs = [(i, (i + shift) % count) for i in range(count)]
            came = lax.ppermute(values, axis, pairs)
            whole = lax.dynamic_update_slice_in_dim(
                whole, came[None], (here + count - shift) % count, 0
            )
        values = whole
    values = values.reshape(2, 4, 2, *values.shape[3:])
    return values.reshape(BLOCKS, *values.shape[3:])


def swap_pairs():
    pairs = []
    for row in range(BLOCKS):
        for col in range(SUPERS):
            half, odd = row // 2, row % 2
            if half == col:
                to = (row ^ 1, col)
            elif half < col:
                to = (2 * col + odd, half)
            else:
                to = (2 * col + 1 - odd, half)
            pairs.append((row * SUPERS + col, to[0] * SUPERS + to[1]))
    return pairs


def local(
    local_inverse,
    coupling,
    local_rhs,
    members,
    shared_matrix,
    shared_rhs,
    prior_solution,
    preconditioner,
):
    core = lax.axis_index("core")
    row = lax.axis_index(AXES[:3])
    col = lax.axis_index(COL)
    place = jnp.stack([core, row, col]).astype(jnp.int32)
    both = gathered(jnp.stack([prior_solution, preconditioner]))
    prior, scale = both[:, 0:1], both[:, 1:2]
    start = lax.dynamic_slice_in_dim(prior.reshape(-1), col * 2 * BLOCK, 2 * BLOCK)
    base = jnp.where(col == 0, shared_rhs, 0.0) - jnp.dot(
        shared_matrix, start, precision=lax.Precision.HIGHEST, preferred_element_type=F32
    )
    diag = jnp.zeros((SUPERS, 8, BLOCK), F32)
    pieces = []
    for number, (first, rows) in enumerate(CHUNKS):
        last = number == len(CHUNKS) - 1
        out = eliminate(
            first,
            rows,
            last,
            members,
            place,
            local_inverse,
            coupling,
            diag,
            local_rhs[:, None, :],
            prior,
            base[None],
        )
        keep, send = out[:2]
        if not last:
            diag = out[2]
        came = lax.ppermute(send, "core", [(0, 1), (1, 0)])
        spread = lax.all_to_all(keep + came, CHIP_AXES, 0, 0, tiled=True)
        pieces.append(jnp.sum(spread, axis=0))
    own = jnp.concatenate(pieces, axis=0)
    other = lax.ppermute(own, AXES, swap_pairs())
    matrix, rhs, product, known = own_tile(
        place, own, other, shared_matrix, shared_rhs[None], prior, scale
    )
    products = lax.all_to_all(
        jnp.broadcast_to(product[0:1], (SUPERS, BLOCK)), COL, 0, 0, tiled=True
    )
    rhs = rhs[0]
    solution = known[0] + preconditioner * (rhs - jnp.sum(products, axis=0))
    return (matrix, rhs, solution)


def solution(mesh):
    finer = Mesh(mesh.devices.reshape(2, 4, 2, 2, 4), AXES)
    weeks = P(AXES)
    rows = P(AXES[:3])
    tiles = P(AXES[:3], COL)
    return jax.shard_map(
        local,
        mesh=finer,
        in_specs=(weeks, weeks, weeks, weeks, tiles, rows, rows, rows),
        out_specs=(tiles, rows, rows),
        check_vma=False,
    )
```

```python
import functools

import jax
import jax.numpy as jnp
from jax import lax
from jax.experimental import pallas as pl
from jax.experimental.pallas import tpu as pltpu
from jax.sharding import Mesh
from jax.sharding import PartitionSpec as P

BLOCK = 128
BLOCKS = 16
TOUCHED = 8
PAIRS = TOUCHED // 2
SUPERS = BLOCKS // 2
CHIPS = 64
EXTRA = 16
PIECE = 144
HALF = PIECE // 2
PARTS = (
    (("x_hi", "x_lo"), False, 0, 16),
    (("x_hi", "x_lo"), True, 16, 8),
    (("y",), False, 24, 16),
    (("y",), True, 40, 8),
    (("z",), False, 48, 16),
    (("z",), True, 64, 8),
)

AXES = ("x_hi", "z", "core", "x_lo", "y")
CHIP_AXES = ("x_hi", "z", "x_lo", "y")
COL = ("x_lo", "y")
F32 = jnp.float32
BF16 = jnp.bfloat16


def halves(values):
    high = values.astype(BF16)
    return high, (values - high.astype(F32)).astype(BF16)


def mul(left, right):
    return lax.dot_general(left, right, (((1,), (0,)), ((), ())), preferred_element_type=F32)


def place_of(low, high, core):
    low_super, low_odd = low // 2, low % 2
    high_super, high_odd = high // 2, high % 2
    same = low_odd == high_odd
    upper = jnp.logical_or(same, low_super == high_super)
    odd = jnp.where(low_super == high_super, 1, jnp.where(same, low_odd, high_odd))
    row = jnp.where(upper, low_super, high_super)
    column = jnp.where(upper, high_super, low_super)
    return (odd ^ core) * CHIPS + row * SUPERS + column


def eliminate_kernel(members, place, inverse, coupling, rhs, prior, shared, shared_rhs, *refs):
    count = len(PARTS)
    keep, send, refs = refs[:count], refs[count : 2 * count], refs[2 * count :]
    packed, vec, diag, sems = refs[:4]
    slots = (refs[4:13], refs[13:22])
    mh, ml = refs[22:24]
    weeks, size, _ = inverse.shape
    core = place[0]

    def fetch(week, side, copy=True):
        inverse_in, coupling_in = slots[side][:2]
        week = jnp.minimum(week, weeks - 1)
        copies = (
            pltpu.make_async_copy(inverse.at[week], inverse_in, sems.at[2 * side]),
            pltpu.make_async_copy(coupling.at[week], coupling_in, sems.at[2 * side + 1]),
        )
        for one in copies:
            if copy:
                one.start()
            else:
                one.wait()

    def order(week, side):
        ordered = slots[side][-1]
        blocks = [members[week, slot] for slot in range(TOUCHED)]
        ranks = []
        for slot in range(TOUCHED):
            rank = jnp.int32(0)
            for other in range(TOUCHED):
                if other != slot:
                    rank = rank + (blocks[other] < blocks[slot]).astype(jnp.int32)
            ordered[rank] = blocks[slot]
            ranks.append(rank)
        return blocks, ranks

    def prepare(week, side, blocks, ranks):
        inverse_in, coupling_in, ch, cl, ah, al, lh, ll, _ = slots[side]
        image = []

        def column(slot):
            tile = coupling_in[:, slot * BLOCK : (slot + 1) * BLOCK]
            high, low = halves(tile)
            at = pl.ds(pl.multiple_of(ranks[slot] * BLOCK, BLOCK), BLOCK)
            ch[:, at] = high
            cl[:, at] = low
            turned_high, turned_low = halves(tile.T)
            at = pl.ds(pl.multiple_of(EXTRA + ranks[slot] * BLOCK, 16), BLOCK)
            lh[at, :] = turned_high
            ll[at, :] = turned_low
            part = tile * prior[blocks[slot]]
            image[:] = [image[0] + part] if image else [part]
            if slot == TOUCHED - 1:
                lead = jnp.sum(image[0].T, axis=0, keepdims=True)
                week_rhs = rhs[pl.ds(week, 1), :]
                index = lax.broadcasted_iota(jnp.int32, (EXTRA, size), 0)
                lead = jnp.where(
                    index == 0, week_rhs, jnp.where(index == 1, lead - week_rhs, 0.0)
                )
                lead_high, lead_low = halves(lead)
                lh[:EXTRA, :] = lead_high
                ll[:EXTRA, :] = lead_low

        def square(part):
            at = slice(part * size // 2, (part + 1) * size // 2)
            high, low = halves(inverse_in[at, :])
            ah[at, :] = high
            al[at, :] = low

        steps = [functools.partial(column, slot) for slot in range(TOUCHED)]
        return steps + [functools.partial(square, part) for part in range(2)]

    def products(side, steps):
        _, _, ch, cl, ah, al, lh, ll, ordered = slots[side]
        steps = list(steps)

        def step(count):
            for _ in range(count):
                if steps:
                    steps.pop(0)()

        step(1)
        for part in range(2):
            at = slice(part * size // 2, (part + 1) * size // 2)
            a_high, a_low = ah[:, at], al[:, at]
            mapped = mul(lh[...], a_high) + mul(ll[...], a_high) + mul(lh[...], a_low)
            high, low = halves(mapped)
            mh[:, at] = high
            ml[:, at] = low
            step(2)
        row = lax.broadcasted_iota(jnp.int32, (BLOCK, BLOCK), 0)
        column = lax.broadcasted_iota(jnp.int32, (BLOCK, BLOCK), 1)
        for pair in range(PAIRS):
            count = EXTRA + (2 * pair + 2) * BLOCK
            at = slice(pair * 2 * BLOCK, (pair + 1) * 2 * BLOCK)
            c_high, c_low = ch[:, at], cl[:, at]
            sums = mul(mh[:count], c_high) + mul(ml[:count], c_high) + mul(mh[:count], c_low)
            for right in range(2):
                b = 2 * pair + right
                block = ordered[b]
                vec[block, 0:8, :] += sums[:8, right * BLOCK : (right + 1) * BLOCK]
                for a in range(b + 1):
                    tile = sums[
                        EXTRA + a * BLOCK : EXTRA + (a + 1) * BLOCK,
                        right * BLOCK : (right + 1) * BLOCK,
                    ]
                    if a == b:
                        odd = block % 2
                        own = (core * CHIPS) + (block // 2) * (SUPERS + 1)
                        upper = (row <= column).astype(jnp.int32)
                        packed[own, :BLOCK, :] += jnp.where(upper != odd, tile, 0.0)
                        line = jnp.sum(
                            jnp.where(row == column, tile, 0.0), axis=0, keepdims=True
                        ) * odd.astype(F32)
                        diag[block // 2, 0:1, :] += line
                    else:
                        own = place_of(ordered[a], block, core)
                        packed[own, :BLOCK, :] += tile
            step(1 + pair // 2)
        step(len(steps))

    fetch(0, 0)
    fetch(1, 1)
    packed[...] = jnp.zeros_like(packed)
    diag[...] = jnp.zeros_like(diag)
    vec[...] = jnp.zeros_like(vec)
    blocks, ranks = order(0, 0)
    fetch(0, 0, copy=False)
    for one in prepare(0, 0, blocks, ranks):
        one()
    fetch(2, 0)

    def two_weeks(number, carry):
        for side in range(2):
            week = jnp.minimum(2 * number + side + 1, weeks - 1)
            blocks, ranks = order(week, 1 - side)
            fetch(week, 1 - side, copy=False)
            products(side, prepare(week, 1 - side, blocks, ranks))
            fetch(week + 2, 1 - side)
        return carry

    lax.fori_loop(0, weeks // 2, two_weeks, 0)
    fetch(weeks, 0, copy=False)
    fetch(weeks, 1, copy=False)
    mine, col = place[1], place[2]
    image = shared[:, :BLOCK] * prior[2 * col] + shared[:, BLOCK:] * prior[2 * col + 1]
    base = shared_rhs[...] * (col == 0).astype(F32) - jnp.sum(image.T, axis=0, keepdims=True)
    vec[mine, 1:2, :] += base
    for odd in range(2):
        for chip_row in range(SUPERS):
            own = vec[2 * chip_row + odd, 0:2, :]
            for col in range(SUPERS):
                at = (odd ^ core) * CHIPS + chip_row * SUPERS + col
                packed[at, BLOCK : BLOCK + 2, :] = own
                packed[at, BLOCK + 2 : BLOCK + 3, :] = vec[2 * col, 1:2, :]
                packed[at, BLOCK + 3 : BLOCK + 4, :] = vec[2 * col + 1, 1:2, :]
                if odd == 0 and chip_row == col:
                    packed[at, BLOCK + 4 : BLOCK + 5, :] = diag[col, 0:1, :]
    copies = []
    for half, outs in ((1, send), (0, keep)):
        for (_, _, first, rows), out in zip(PARTS, outs):
            for bit in range(2):
                source = packed.at[
                    pl.ds(half * CHIPS, CHIPS), pl.ds(bit * HALF + first, rows), :
                ]
                copies.append(
                    pltpu.make_async_copy(
                        source, out.at[:, pl.ds(bit * rows, rows), :], sems.at[4 + len(copies)]
                    )
                )
    for copy in copies:
        copy.start()
    for copy in copies:
        copy.wait()


def eliminate(members, place, inverse, coupling, rhs, prior, shared, shared_rhs):
    weeks, size, width = coupling.shape
    count = EXTRA + width
    pieces = [jax.ShapeDtypeStruct((CHIPS, 2 * part[3], BLOCK), F32) for part in PARTS] * 2
    smem = pl.BlockSpec(memory_space=pltpu.SMEM)
    vmem = pl.BlockSpec(memory_space=pltpu.VMEM)
    hbm = pl.BlockSpec(memory_space=pl.ANY)
    scratch = [
        pltpu.VMEM((2 * CHIPS, PIECE, BLOCK), F32),
        pltpu.VMEM((BLOCKS, 8, BLOCK), F32),
        pltpu.VMEM((SUPERS, 8, BLOCK), F32),
        pltpu.SemaphoreType.DMA((4 + 4 * len(PARTS),)),
    ]
    for _ in range(2):
        scratch += [
            pltpu.VMEM((size, size), F32),
            pltpu.VMEM((size, width), F32),
            pltpu.VMEM((size, width), BF16),
            pltpu.VMEM((size, width), BF16),
            pltpu.VMEM((size, size), BF16),
            pltpu.VMEM((size, size), BF16),
            pltpu.VMEM((count, size), BF16),
            pltpu.VMEM((count, size), BF16),
            pltpu.SMEM((TOUCHED,), jnp.int32),
        ]
    scratch += [pltpu.VMEM((count, size), BF16), pltpu.VMEM((count, size), BF16)]
    return pl.pallas_call(
        eliminate_kernel,
        out_shape=pieces,
        in_specs=[smem, smem, hbm, hbm, vmem, vmem, vmem, vmem],
        out_specs=[hbm] * len(pieces),
        scratch_shapes=scratch,
        compiler_params=pltpu.CompilerParams(vmem_limit_bytes=58 * 1024 * 1024),
        cost_estimate=pl.CostEstimate(
            flops=weeks * 2 * 3 * width * size * (size + 640),
            bytes_accessed=weeks * size * (size + width) * 4,
            transcendentals=0,
        ),
        name="eliminate",
    )(members, place, inverse, coupling, rhs, prior, shared, shared_rhs)


def collect_kernel(spread, piece):
    for axes, crossed, first, rows in PARTS:
        at = slice(first, first + rows)
        for bit in range(2):
            total = None
            for chip in range(CHIPS):
                if chip_bit(axes, crossed, chip) == bit:
                    came = spread[chip, at, :]
                    total = came if total is None else total + came
            piece[bit * HALF + first : bit * HALF + first + rows, :] = total


def chip_bit(axes, crossed, chip):
    x_hi, z, x_lo, y = chip // 32, chip // 8 % 4, chip // 4 % 2, chip % 4
    at = {"y": y, "z": z}.get(axes[0], 2 * x_hi + x_lo)
    return at // 2 if crossed else at % 2


def collect(spread):
    vmem = pl.BlockSpec(memory_space=pltpu.VMEM)
    return pl.pallas_call(
        collect_kernel,
        out_shape=jax.ShapeDtypeStruct((PIECE, BLOCK), F32),
        in_specs=[vmem],
        out_specs=vmem,
        name="collect",
    )(spread)


def tile_kernel(place, own, other, shared, shared_rhs, prior, scale, matrix, rhs, product, known):
    mine, col = place[1], place[2]
    odd = mine % 2
    half = mine // 2
    upper, lower, level = half < col, half > col, half == col
    first, second = own[:BLOCK, :], other[:BLOCK, :]
    first_turned, second_turned = first.T, second.T
    row = lax.broadcasted_iota(jnp.int32, (BLOCK, BLOCK), 0)
    column = lax.broadcasted_iota(jnp.int32, (BLOCK, BLOCK), 1)
    even_tile = jnp.where(row <= column, first, first_turned)
    odd_tile = jnp.where(
        row > column,
        second,
        jnp.where(row == column, other[BLOCK + 4 : BLOCK + 5, :], second_turned),
    )
    level_even = jnp.logical_and(level, odd == 0)
    level_odd = jnp.logical_and(level, odd == 1)
    turn = jnp.logical_or(lower, level_odd)
    own_tile = jnp.where(level_even, even_tile, jnp.where(turn, first_turned, first))
    other_tile = jnp.where(level_odd, odd_tile, jnp.where(lower, second_turned, second))
    own_left = jnp.logical_or(
        level, jnp.logical_or(jnp.logical_and(upper, odd == 0), jnp.logical_and(lower, odd == 1))
    )
    left = shared[:, :BLOCK] - jnp.where(own_left, own_tile, other_tile)
    right = shared[:, BLOCK:] - jnp.where(own_left, other_tile, own_tile)
    matrix[:, :BLOCK] = left
    matrix[:, BLOCK:] = right
    rhs[...] = shared_rhs[...] - own[BLOCK : BLOCK + 1, :]
    known[...] = prior[mine] + scale[mine] * own[BLOCK + 1 : BLOCK + 2, :]
    left_known = prior[2 * col] + scale[2 * col] * own[BLOCK + 2 : BLOCK + 3, :]
    right_known = prior[2 * col + 1] + scale[2 * col + 1] * own[BLOCK + 3 : BLOCK + 4, :]
    dims = (((1,), (1,)), ((), ()))
    times = functools.partial(
        lax.dot_general,
        dimension_numbers=dims,
        precision=lax.Precision.HIGHEST,
        preferred_element_type=F32,
    )
    left_known = jnp.broadcast_to(left_known, (8, BLOCK))
    right_known = jnp.broadcast_to(right_known, (8, BLOCK))
    product[...] = times(left_known, left) + times(right_known, right)


def own_tile(place, own, other, shared, shared_rhs, prior, scale):
    vmem = pl.BlockSpec(memory_space=pltpu.VMEM)
    line = jax.ShapeDtypeStruct((1, BLOCK), F32)
    return pl.pallas_call(
        tile_kernel,
        out_shape=[
            jax.ShapeDtypeStruct(shared.shape, F32),
            line,
            jax.ShapeDtypeStruct((8, BLOCK), F32),
            line,
        ],
        in_specs=[pl.BlockSpec(memory_space=pltpu.SMEM)] + [vmem] * 6,
        out_specs=[vmem] * 4,
        name="own_tile",
    )(place, own, other, shared, shared_rhs, prior, scale)


def gathered(values):
    copies = jnp.broadcast_to(values[None], (BLOCKS, *values.shape))
    return lax.all_to_all(copies, AXES[:3], 0, 0, tiled=True)


def halved(keep, send):
    came = [lax.ppermute(part, "core", [(0, 1), (1, 0)]) for part in send]

    def half(number, bit):
        rows = PARTS[number][3]
        return lax.dynamic_slice_in_dim(
            keep[number], bit * rows, rows, 1
        ) + lax.dynamic_slice_in_dim(came[number], bit * rows, rows, 1)

    bits, got = [], []
    for number, (axes, crossed, _, _) in enumerate(PARTS):
        here = lax.axis_index(axes)
        bits.append(here // 2 if crossed else here % 2)
        pairs = [(i, 3 - i if crossed else i ^ 1) for i in range(4)]
        got.append(lax.ppermute(half(number, 1 - bits[number]), axes, pairs))
    parts = [half(number, bits[number]) + got[number] for number in range(len(PARTS))]
    return jnp.concatenate(parts, axis=1)


def swap_pairs():
    pairs = []
    for row in range(BLOCKS):
        for col in range(SUPERS):
            half, odd = row // 2, row % 2
            if half == col:
                to = (row ^ 1, col)
            elif half < col:
                to = (2 * col + odd, half)
            else:
                to = (2 * col + 1 - odd, half)
            pairs.append((row * SUPERS + col, to[0] * SUPERS + to[1]))
    return pairs


def local(
    local_inverse,
    coupling,
    local_rhs,
    members,
    shared_matrix,
    shared_rhs,
    prior_solution,
    preconditioner,
):
    core = lax.axis_index("core")
    row = lax.axis_index(AXES[:3])
    col = lax.axis_index(COL)
    place = jnp.stack([core, row, col]).astype(jnp.int32)
    both = gathered(jnp.stack([prior_solution, preconditioner]))
    prior, scale = both[:, 0:1], both[:, 1:2]
    pieces = eliminate(
        members,
        place,
        local_inverse,
        coupling,
        local_rhs,
        prior,
        shared_matrix,
        shared_rhs[None],
    )
    mixed = halved(pieces[: len(PARTS)], pieces[len(PARTS) :])
    spread = lax.all_to_all(mixed, CHIP_AXES, 0, 0, tiled=True)
    own = collect(spread)
    other = lax.ppermute(own, AXES, swap_pairs())
    matrix, rhs, product, known = own_tile(
        place, own, other, shared_matrix, shared_rhs[None], prior, scale
    )
    products = lax.all_to_all(
        jnp.broadcast_to(product[0:1], (SUPERS, BLOCK)), COL, 0, 0, tiled=True
    )
    rhs = rhs[0]
    solution = known[0] + preconditioner * (rhs - jnp.sum(products, axis=0))
    return (matrix, rhs, solution)


def solution(mesh):
    finer = Mesh(mesh.devices.reshape(2, 4, 2, 2, 4), AXES)
    weeks = P(AXES)
    rows = P(AXES[:3])
    tiles = P(AXES[:3], COL)
    return jax.shard_map(
        local,
        mesh=finer,
        in_specs=(weeks, weeks, weeks, weeks, tiles, rows, rows, rows),
        out_specs=(tiles, rows, rows),
        check_vma=False,
    )
```

```python
import functools

import jax
import jax.numpy as jnp
from jax import lax
from jax.experimental import pallas as pl
from jax.experimental.pallas import tpu as pltpu
from jax.sharding import Mesh
from jax.sharding import PartitionSpec as P

BLOCK = 128
BLOCKS = 16
TOUCHED = 8
PAIRS = TOUCHED // 2
SUPERS = BLOCKS // 2
CHIPS = 64
EXTRA = 16
PIECE = 144
HALF = PIECE // 2
PARTS = (
    (("x_hi", "x_lo"), False, 0, 16),
    (("x_hi", "x_lo"), True, 16, 8),
    (("y",), False, 24, 16),
    (("y",), True, 40, 8),
    (("z",), False, 48, 16),
    (("z",), True, 64, 8),
)

AXES = ("x_hi", "z", "core", "x_lo", "y")
CHIP_AXES = ("x_hi", "z", "x_lo", "y")
COL = ("x_lo", "y")
F32 = jnp.float32
BF16 = jnp.bfloat16


def halves(values):
    high = values.astype(BF16)
    return high, (values - high.astype(F32)).astype(BF16)


def mul(left, right):
    return lax.dot_general(left, right, (((1,), (0,)), ((), ())), preferred_element_type=F32)


def place_of(low, high, core):
    low_super, low_odd = low // 2, low % 2
    high_super, high_odd = high // 2, high % 2
    same = low_odd == high_odd
    upper = jnp.logical_or(same, low_super == high_super)
    odd = jnp.where(low_super == high_super, 1, jnp.where(same, low_odd, high_odd))
    row = jnp.where(upper, low_super, high_super)
    column = jnp.where(upper, high_super, low_super)
    return (odd ^ core) * CHIPS + row * SUPERS + column


def eliminate_kernel(
    members, place, inverse, coupling, rhs, prior, scale, shared, shared_rhs, *refs
):
    parts = len(PARTS)
    keep, send, refs = refs[:parts], refs[parts : 2 * parts], refs[2 * parts :]
    packed, vec, diag, ranks, ordered, sems = refs[:6]
    slots = (refs[6:16], refs[16:26])
    weeks, size, _ = inverse.shape
    core = place[0]

    def fetch(week, side, copy=True):
        inverse_in, coupling_in = slots[side][:2]
        copies = (
            pltpu.make_async_copy(inverse.at[week], inverse_in, sems.at[2 * side]),
            pltpu.make_async_copy(coupling.at[week], coupling_in, sems.at[2 * side + 1]),
        )
        for one in copies:
            if copy:
                one.start()
            else:
                one.wait()

    def order(week):
        blocks = [members[week, slot] for slot in range(TOUCHED)]
        for slot in range(TOUCHED):
            rank = jnp.int32(0)
            for other in range(TOUCHED):
                if other != slot:
                    rank = rank + (blocks[other] < blocks[slot]).astype(jnp.int32)
            ranks[week, slot] = rank
            ordered[week, rank] = blocks[slot]

    def prepare(week, side):
        inverse_in, coupling_in, ch, cl, ah, al, lh, ll, _, _ = slots[side]
        image = []

        def column(slot):
            tile = coupling_in[:, slot * BLOCK : (slot + 1) * BLOCK]
            rank = ranks[week, slot]
            high, low = halves(tile)
            at = pl.ds(pl.multiple_of(rank * BLOCK, BLOCK), BLOCK)
            ch[:, at] = high
            cl[:, at] = low
            at = pl.ds(pl.multiple_of(EXTRA + rank * BLOCK, 16), BLOCK)
            lh[at, :] = high.T
            ll[at, :] = low.T
            part = tile * prior[pl.ds(members[week, slot], 1), :]
            image[:] = [image[0] + part] if image else [part]
            if slot == TOUCHED - 1:
                lead = jnp.sum(image[0].T, axis=0, keepdims=True)
                week_rhs = rhs[pl.ds(week, 1), :]
                index = lax.broadcasted_iota(jnp.int32, (EXTRA, size), 0)
                lead = jnp.where(
                    index == 0, week_rhs, jnp.where(index == 1, lead - week_rhs, 0.0)
                )
                lead_high, lead_low = halves(lead)
                lh[:EXTRA, :] = lead_high
                ll[:EXTRA, :] = lead_low

        def square(part):
            at = slice(part * size // 2, (part + 1) * size // 2)
            high, low = halves(inverse_in[at, :])
            ah[at, :] = high
            al[at, :] = low

        steps = [functools.partial(square, part) for part in range(2)]
        return steps + [functools.partial(column, slot) for slot in range(TOUCHED)]

    def map_week(side):
        _, _, _, _, ah, al, lh, ll, mh, ml = slots[side]
        middle = EXTRA + TOUCHED // 2 * BLOCK
        for at in (slice(0, middle), slice(middle, EXTRA + TOUCHED * BLOCK)):
            for part in range(2):
                to = slice(part * size // 2, (part + 1) * size // 2)
                a_high, a_low = ah[:, to], al[:, to]
                mapped = mul(lh[at, :], a_high) + mul(ll[at, :], a_high) + mul(lh[at, :], a_low)
                high, low = halves(mapped)
                mh[at, to] = high
                ml[at, to] = low

    def contribute(week, side, steps):
        _, _, ch, cl, _, _, _, _, mh, ml = slots[side]
        steps = list(steps)
        row = lax.broadcasted_iota(jnp.int32, (BLOCK, BLOCK), 0)
        column = lax.broadcasted_iota(jnp.int32, (BLOCK, BLOCK), 1)
        for pair in range(PAIRS):
            count = EXTRA + (2 * pair + 2) * BLOCK
            at = slice(pair * 2 * BLOCK, (pair + 1) * 2 * BLOCK)
            c_high, c_low = ch[:, at], cl[:, at]
            sums = mul(mh[:count], c_high) + mul(ml[:count], c_high) + mul(mh[:count], c_low)
            for _ in range(pair + 1):
                if steps:
                    steps.pop(0)()
            for right in range(2):
                b = 2 * pair + right
                block = ordered[week, b]
                vec[block, 0:8, :] += sums[:8, right * BLOCK : (right + 1) * BLOCK]
                for a in range(b + 1):
                    tile = sums[
                        EXTRA + a * BLOCK : EXTRA + (a + 1) * BLOCK,
                        right * BLOCK : (right + 1) * BLOCK,
                    ]
                    if a == b:
                        odd = block % 2
                        own = (core * CHIPS) + (block // 2) * (SUPERS + 1)
                        upper = (row <= column).astype(jnp.int32)
                        packed[own, :BLOCK, :] += jnp.where(upper != odd, tile, 0.0)
                        line = jnp.sum(
                            jnp.where(row == column, tile, 0.0), axis=0, keepdims=True
                        ) * odd.astype(F32)
                        diag[block // 2, 0:1, :] += line
                    else:
                        own = place_of(ordered[week, a], block, core)
                        packed[own, :BLOCK, :] += tile
        assert not steps

    def step(week, side, ahead):
        steps = []
        if ahead:
            fetch(week + 1, 1 - side, copy=False)
            steps = prepare(week + 1, 1 - side)
        contribute(week, side, steps)
        if ahead:
            map_week(1 - side)

    fetch(0, 0)
    fetch(1, 1)
    for week in range(weeks):
        order(week)
    packed[...] = jnp.zeros_like(packed)
    diag[...] = jnp.zeros_like(diag)
    vec[...] = jnp.zeros_like(vec)
    fetch(0, 0, copy=False)
    for one in prepare(0, 0):
        one()
    map_week(0)
    fetch(2, 0)

    def two_weeks(number, carry):
        for side in range(2):
            week = 2 * number + side
            step(week, side, True)
            pl.when(week + 3 < weeks)(functools.partial(fetch, week + 3, 1 - side))
        return carry

    lax.fori_loop(0, weeks // 2 - 1, two_weeks, 0)
    step(weeks - 2, 0, True)
    step(weeks - 1, 1, False)
    mine, col = place[1], place[2]
    first = (col == 0).astype(F32)
    image = shared[:, :BLOCK] * prior[pl.ds(2 * col, 1), :]
    image += shared[:, BLOCK:] * prior[pl.ds(2 * col + 1, 1), :]
    base = shared_rhs[...] * first - jnp.sum(image.T, axis=0, keepdims=True)
    vec[mine, 1:2, :] += base
    vec[mine, 2:3, :] = scale[...] * first
    for odd in range(2):
        for chip_row in range(SUPERS):
            own = vec[2 * chip_row + odd, 0:2, :]
            for col in range(SUPERS):
                at = (odd ^ core) * CHIPS + chip_row * SUPERS + col
                packed[at, BLOCK : BLOCK + 2, :] = own
                packed[at, BLOCK + 2 : BLOCK + 4, :] = vec[2 * col, 1:3, :]
                packed[at, BLOCK + 4 : BLOCK + 6, :] = vec[2 * col + 1, 1:3, :]
                if odd == 0 and chip_row == col:
                    packed[at, BLOCK + 6 : BLOCK + 7, :] = diag[col, 0:1, :]
    copies = []
    for half, outs in ((1, send), (0, keep)):
        for (_, _, first, rows), out in zip(PARTS, outs):
            for bit in range(2):
                source = packed.at[
                    pl.ds(half * CHIPS, CHIPS), pl.ds(bit * HALF + first, rows), :
                ]
                copies.append(
                    pltpu.make_async_copy(
                        source, out.at[:, pl.ds(bit * rows, rows), :], sems.at[4 + len(copies)]
                    )
                )
    for copy in copies:
        copy.start()
    for copy in copies:
        copy.wait()


def eliminate(members, place, inverse, coupling, rhs, prior, scale, shared, shared_rhs):
    weeks, size, width = coupling.shape
    count = EXTRA + width
    pieces = [jax.ShapeDtypeStruct((CHIPS, 2 * part[3], BLOCK), F32) for part in PARTS] * 2
    smem = pl.BlockSpec(memory_space=pltpu.SMEM)
    vmem = pl.BlockSpec(memory_space=pltpu.VMEM)
    hbm = pl.BlockSpec(memory_space=pl.ANY)
    scratch = [
        pltpu.VMEM((2 * CHIPS, PIECE, BLOCK), F32),
        pltpu.VMEM((BLOCKS, 8, BLOCK), F32),
        pltpu.VMEM((SUPERS, 8, BLOCK), F32),
        pltpu.SMEM((weeks, TOUCHED), jnp.int32),
        pltpu.SMEM((weeks, TOUCHED), jnp.int32),
        pltpu.SemaphoreType.DMA((4 + 4 * len(PARTS),)),
    ]
    for _ in range(2):
        scratch += [
            pltpu.VMEM((size, size), F32),
            pltpu.VMEM((size, width), F32),
            pltpu.VMEM((size, width), BF16),
            pltpu.VMEM((size, width), BF16),
            pltpu.VMEM((size, size), BF16),
            pltpu.VMEM((size, size), BF16),
        ] + [pltpu.VMEM((count, size), BF16)] * 4
    return pl.pallas_call(
        eliminate_kernel,
        out_shape=pieces,
        in_specs=[smem, smem, hbm, hbm] + [vmem] * 5,
        out_specs=[hbm] * len(pieces),
        scratch_shapes=scratch,
        compiler_params=pltpu.CompilerParams(vmem_limit_bytes=58 * 1024 * 1024),
        cost_estimate=pl.CostEstimate(
            flops=weeks * 2 * 3 * width * size * (size + 640),
            bytes_accessed=weeks * size * (size + width) * 4,
            transcendentals=0,
        ),
        name="eliminate",
    )(members, place, inverse, coupling, rhs, prior, scale, shared, shared_rhs)


def collect_kernel(spread, piece):
    for axes, crossed, first, rows in PARTS:
        at = slice(first, first + rows)
        for bit in range(2):
            total = None
            for chip in range(CHIPS):
                if chip_bit(axes, crossed, chip) == bit:
                    came = spread[chip, at, :]
                    total = came if total is None else total + came
            piece[bit * HALF + first : bit * HALF + first + rows, :] = total


def chip_bit(axes, crossed, chip):
    x_hi, z, x_lo, y = chip // 32, chip // 8 % 4, chip // 4 % 2, chip % 4
    at = {"y": y, "z": z}.get(axes[0], 2 * x_hi + x_lo)
    return at // 2 if crossed else at % 2


def collect(spread):
    vmem = pl.BlockSpec(memory_space=pltpu.VMEM)
    return pl.pallas_call(
        collect_kernel,
        out_shape=jax.ShapeDtypeStruct((PIECE, BLOCK), F32),
        in_specs=[vmem],
        out_specs=vmem,
        name="collect",
    )(spread)


def tile_kernel(place, own, other, shared, shared_rhs, prior, scale, matrix, rhs, product, known):
    mine, col = place[1], place[2]
    odd = mine % 2
    half = mine // 2
    upper, lower, level = half < col, half > col, half == col
    first, second = own[:BLOCK, :], other[:BLOCK, :]
    first_turned, second_turned = first.T, second.T
    row = lax.broadcasted_iota(jnp.int32, (BLOCK, BLOCK), 0)
    column = lax.broadcasted_iota(jnp.int32, (BLOCK, BLOCK), 1)
    even_tile = jnp.where(row <= column, first, first_turned)
    odd_tile = jnp.where(
        row > column,
        second,
        jnp.where(row == column, other[BLOCK + 6 : BLOCK + 7, :], second_turned),
    )
    level_even = jnp.logical_and(level, odd == 0)
    level_odd = jnp.logical_and(level, odd == 1)
    turn = jnp.logical_or(lower, level_odd)
    own_tile = jnp.where(level_even, even_tile, jnp.where(turn, first_turned, first))
    other_tile = jnp.where(level_odd, odd_tile, jnp.where(lower, second_turned, second))
    own_left = jnp.logical_or(
        level, jnp.logical_or(jnp.logical_and(upper, odd == 0), jnp.logical_and(lower, odd == 1))
    )
    left = shared[:, :BLOCK] - jnp.where(own_left, own_tile, other_tile)
    right = shared[:, BLOCK:] - jnp.where(own_left, other_tile, own_tile)
    matrix[:, :BLOCK] = left
    matrix[:, BLOCK:] = right
    rhs[...] = shared_rhs[...] - own[BLOCK : BLOCK + 1, :]
    known[...] = prior[pl.ds(mine, 1), :] + scale[...] * own[BLOCK + 1 : BLOCK + 2, :]
    left_known = prior[pl.ds(2 * col, 1), :]
    left_known += own[BLOCK + 3 : BLOCK + 4, :] * own[BLOCK + 2 : BLOCK + 3, :]
    right_known = prior[pl.ds(2 * col + 1, 1), :]
    right_known += own[BLOCK + 5 : BLOCK + 6, :] * own[BLOCK + 4 : BLOCK + 5, :]
    dims = (((1,), (1,)), ((), ()))
    times = functools.partial(
        lax.dot_general,
        dimension_numbers=dims,
        precision=lax.Precision.HIGHEST,
        preferred_element_type=F32,
    )
    left_known = jnp.broadcast_to(left_known, (8, BLOCK))
    right_known = jnp.broadcast_to(right_known, (8, BLOCK))
    product[...] = times(left_known, left) + times(right_known, right)


def own_tile(place, own, other, shared, shared_rhs, prior, scale):
    vmem = pl.BlockSpec(memory_space=pltpu.VMEM)
    line = jax.ShapeDtypeStruct((1, BLOCK), F32)
    return pl.pallas_call(
        tile_kernel,
        out_shape=[
            jax.ShapeDtypeStruct(shared.shape, F32),
            line,
            jax.ShapeDtypeStruct((8, BLOCK), F32),
            line,
        ],
        in_specs=[pl.BlockSpec(memory_space=pltpu.SMEM)] + [vmem] * 6,
        out_specs=[vmem] * 4,
        name="own_tile",
    )(place, own, other, shared, shared_rhs, prior, scale)


def gathered(values):
    copies = jnp.broadcast_to(values[None], (BLOCKS, *values.shape))
    return lax.all_to_all(copies, AXES[:3], 0, 0, tiled=True)


def halved(keep, send):
    came = [lax.ppermute(part, "core", [(0, 1), (1, 0)]) for part in send]

    def half(number, bit):
        rows = PARTS[number][3]
        return lax.dynamic_slice_in_dim(
            keep[number], bit * rows, rows, 1
        ) + lax.dynamic_slice_in_dim(came[number], bit * rows, rows, 1)

    bits, got = [], []
    for number, (axes, crossed, _, _) in enumerate(PARTS):
        here = lax.axis_index(axes)
        bits.append(here // 2 if crossed else here % 2)
        pairs = [(i, 3 - i if crossed else i ^ 1) for i in range(4)]
        got.append(lax.ppermute(half(number, 1 - bits[number]), axes, pairs))
    parts = [half(number, bits[number]) + got[number] for number in range(len(PARTS))]
    return jnp.concatenate(parts, axis=1)


def swap_pairs():
    pairs = []
    for row in range(BLOCKS):
        for col in range(SUPERS):
            half, odd = row // 2, row % 2
            if half == col:
                to = (row ^ 1, col)
            elif half < col:
                to = (2 * col + odd, half)
            else:
                to = (2 * col + 1 - odd, half)
            pairs.append((row * SUPERS + col, to[0] * SUPERS + to[1]))
    return pairs


def local(
    local_inverse,
    coupling,
    local_rhs,
    members,
    shared_matrix,
    shared_rhs,
    prior_solution,
    preconditioner,
):
    core = lax.axis_index("core")
    row = lax.axis_index(AXES[:3])
    col = lax.axis_index(COL)
    place = jnp.stack([core, row, col]).astype(jnp.int32)
    prior = gathered(prior_solution)
    scale = preconditioner[None]
    pieces = eliminate(
        members,
        place,
        local_inverse,
        coupling,
        local_rhs,
        prior,
        scale,
        shared_matrix,
        shared_rhs[None],
    )
    mixed = halved(pieces[: len(PARTS)], pieces[len(PARTS) :])
    spread = lax.all_to_all(mixed, CHIP_AXES, 0, 0, tiled=True)
    own = collect(spread)
    other = lax.ppermute(own, AXES, swap_pairs())
    matrix, rhs, product, known = own_tile(
        place, own, other, shared_matrix, shared_rhs[None], prior, scale
    )
    products = lax.all_to_all(product, COL, 0, 0, tiled=True)
    rhs = rhs[0]
    solution = known[0] + preconditioner * (rhs - jnp.sum(products, axis=0))
    return (matrix, rhs, solution)


def solution(mesh):
    finer = Mesh(mesh.devices.reshape(2, 4, 2, 2, 4), AXES)
    weeks = P(AXES)
    rows = P(AXES[:3])
    tiles = P(AXES[:3], COL)
    return jax.shard_map(
        local,
        mesh=finer,
        in_specs=(weeks, weeks, weeks, weeks, tiles, rows, rows, rows),
        out_specs=(tiles, rows, rows),
        check_vma=False,
    )
```

```python
import functools

import jax
import jax.numpy as jnp
from jax import lax
from jax.experimental import pallas as pl
from jax.experimental.pallas import tpu as pltpu
from jax.sharding import Mesh
from jax.sharding import PartitionSpec as P


BLOCK = 128
BLOCKS = 16
TOUCHED = 8
PAIRS = TOUCHED // 2
SUPERS = BLOCKS // 2
CHIPS = 64
EXTRA = 16
TAIL = 8
PIECE = BLOCK + TAIL
HALF = BLOCK // 2
PARTS = (
    (("x_hi", "x_lo"), False, 0, 16),
    (("y",), False, 16, 16),
    (("z",), False, 32, 8),
    (("x_hi", "x_lo"), True, 40, 8),
    (("y",), True, 48, 8),
    (("z",), True, 56, 8),
)
OUTS = len(PARTS) + 1

AXES = ("x_hi", "z", "core", "x_lo", "y")
CHIP_AXES = ("x_hi", "z", "x_lo", "y")
COL = ("x_lo", "y")
F32 = jnp.float32
BF16 = jnp.bfloat16


def halves(values):
    high = values.astype(BF16)
    return high, (values - high.astype(F32)).astype(BF16)


def mul(left, right):
    return lax.dot_general(left, right, (((1,), (0,)), ((), ())), preferred_element_type=F32)


def place_of(low, high, core):
    low_super, low_odd = low // 2, low % 2
    high_super, high_odd = high // 2, high % 2
    same = low_odd == high_odd
    upper = jnp.logical_or(same, low_super == high_super)
    odd = jnp.where(low_super == high_super, 1, jnp.where(same, low_odd, high_odd))
    row = jnp.where(upper, low_super, high_super)
    column = jnp.where(upper, high_super, low_super)
    return (odd ^ core) * CHIPS + row * SUPERS + column


def eliminate_kernel(
    members, place, inverse, coupling, rhs, prior, scale, shared, shared_rhs, *refs
):
    keep, send, refs = refs[:OUTS], refs[OUTS : 2 * OUTS], refs[2 * OUTS :]
    packed, vec, diag, ranks, ordered, sems = refs[:6]
    slots = (refs[6:16], refs[16:26])
    weeks, size, _ = inverse.shape
    core = place[0]

    def fetch(week, side, copy=True):
        inverse_in, coupling_in = slots[side][:2]
        copies = (
            pltpu.make_async_copy(inverse.at[week], inverse_in, sems.at[2 * side]),
            pltpu.make_async_copy(coupling.at[week], coupling_in, sems.at[2 * side + 1]),
        )
        for one in copies:
            if copy:
                one.start()
            else:
                one.wait()

    def order(week):
        blocks = [members[week, slot] for slot in range(TOUCHED)]
        for slot in range(TOUCHED):
            rank = jnp.int32(0)
            for other in range(TOUCHED):
                if other != slot:
                    rank = rank + (blocks[other] < blocks[slot]).astype(jnp.int32)
            ranks[week, slot] = rank
            ordered[week, rank] = blocks[slot]

    def prepare(week, side):
        inverse_in, coupling_in, ch, cl, ah, al, lh, ll, _, _ = slots[side]
        image = []

        def column(slot):
            tile = coupling_in[:, slot * BLOCK : (slot + 1) * BLOCK]
            rank = ranks[week, slot]
            high, low = halves(tile)
            at = pl.ds(pl.multiple_of(rank * BLOCK, BLOCK), BLOCK)
            ch[:, at] = high
            cl[:, at] = low
            at = pl.ds(pl.multiple_of(EXTRA + rank * BLOCK, 16), BLOCK)
            lh[at, :] = high.T
            ll[at, :] = low.T
            part = tile * prior[pl.ds(members[week, slot], 1), :]
            image[:] = [image[0] + part] if image else [part]
            if slot == TOUCHED - 1:
                lead = jnp.sum(image[0].T, axis=0, keepdims=True)
                week_rhs = rhs[pl.ds(week, 1), :]
                index = lax.broadcasted_iota(jnp.int32, (EXTRA, size), 0)
                lead = jnp.where(
                    index == 0, week_rhs, jnp.where(index == 1, lead - week_rhs, 0.0)
                )
                lead_high, lead_low = halves(lead)
                lh[:EXTRA, :] = lead_high
                ll[:EXTRA, :] = lead_low

        def square(part):
            at = slice(part * size // 2, (part + 1) * size // 2)
            high, low = halves(inverse_in[at, :])
            ah[at, :] = high
            al[at, :] = low

        steps = [functools.partial(square, part) for part in range(2)]
        return steps + [functools.partial(column, slot) for slot in range(TOUCHED)]

    def map_week(side):
        _, _, _, _, ah, al, lh, ll, mh, ml = slots[side]
        middle = EXTRA + TOUCHED // 2 * BLOCK
        for at in (slice(0, middle), slice(middle, EXTRA + TOUCHED * BLOCK)):
            for part in range(2):
                to = slice(part * size // 2, (part + 1) * size // 2)
                a_high, a_low = ah[:, to], al[:, to]
                mapped = mul(lh[at, :], a_high) + mul(ll[at, :], a_high) + mul(lh[at, :], a_low)
                high, low = halves(mapped)
                mh[at, to] = high
                ml[at, to] = low

    def contribute(week, side, steps):
        _, _, ch, cl, _, _, _, _, mh, ml = slots[side]
        steps = list(steps)
        row = lax.broadcasted_iota(jnp.int32, (BLOCK, BLOCK), 0)
        column = lax.broadcasted_iota(jnp.int32, (BLOCK, BLOCK), 1)
        for pair in range(PAIRS):
            count = EXTRA + (2 * pair + 2) * BLOCK
            at = slice(pair * 2 * BLOCK, (pair + 1) * 2 * BLOCK)
            c_high, c_low = ch[:, at], cl[:, at]
            sums = mul(mh[:count], c_high) + mul(ml[:count], c_high) + mul(mh[:count], c_low)
            for _ in range(pair + 1):
                if steps:
                    steps.pop(0)()
            for right in range(2):
                b = 2 * pair + right
                block = ordered[week, b]
                vec[block, 0:8, :] += sums[:8, right * BLOCK : (right + 1) * BLOCK]
                for a in range(b + 1):
                    tile = sums[
                        EXTRA + a * BLOCK : EXTRA + (a + 1) * BLOCK,
                        right * BLOCK : (right + 1) * BLOCK,
                    ]
                    if a == b:
                        odd = block % 2
                        own = (core * CHIPS) + (block // 2) * (SUPERS + 1)
                        upper = (row <= column).astype(jnp.int32)
                        packed[own, :BLOCK, :] += jnp.where(upper != odd, tile, 0.0)
                        line = jnp.sum(
                            jnp.where(row == column, tile, 0.0), axis=0, keepdims=True
                        ) * odd.astype(F32)
                        diag[block // 2, 0:1, :] += line
                    else:
                        own = place_of(ordered[week, a], block, core)
                        packed[own, :BLOCK, :] += tile
        assert not steps

    def step(week, side, ahead):
        steps = []
        if ahead:
            fetch(week + 1, 1 - side, copy=False)
            steps = prepare(week + 1, 1 - side)
        contribute(week, side, steps)
        if ahead:
            map_week(1 - side)

    fetch(0, 0)
    for week in range(weeks):
        order(week)
    packed[...] = jnp.zeros_like(packed)
    diag[...] = jnp.zeros_like(diag)
    vec[...] = jnp.zeros_like(vec)
    fetch(0, 0, copy=False)
    fetch(1, 1)
    for one in prepare(0, 0):
        one()
    map_week(0)
    fetch(2, 0)

    def two_weeks(number, carry):
        for side in range(2):
            week = 2 * number + side
            step(week, side, True)
            pl.when(week + 3 < weeks)(functools.partial(fetch, week + 3, 1 - side))
        return carry

    lax.fori_loop(0, weeks // 2 - 1, two_weeks, 0)
    step(weeks - 2, 0, True)
    step(weeks - 1, 1, False)
    mine, col = place[1], place[2]
    first = (col == 0).astype(F32)
    image = shared[:, :BLOCK] * prior[pl.ds(2 * col, 1), :]
    image += shared[:, BLOCK:] * prior[pl.ds(2 * col + 1, 1), :]
    base = shared_rhs[...] * first - jnp.sum(image.T, axis=0, keepdims=True)
    vec[mine, 1:2, :] += base
    vec[mine, 2:3, :] = scale[...] * first
    for odd in range(2):
        for chip_row in range(SUPERS):
            own = vec[2 * chip_row + odd, 0:2, :]
            for col in range(SUPERS):
                at = (odd ^ core) * CHIPS + chip_row * SUPERS + col
                packed[at, BLOCK : BLOCK + 2, :] = own
                packed[at, BLOCK + 2 : BLOCK + 4, :] = vec[2 * col, 1:3, :]
                packed[at, BLOCK + 4 : BLOCK + 6, :] = vec[2 * col + 1, 1:3, :]
                if odd == 0 and chip_row == col:
                    packed[at, BLOCK + 6 : BLOCK + 7, :] = diag[col, 0:1, :]
    copies = []

    def leave(half, first, rows, out, at):
        source = packed.at[pl.ds(half * CHIPS, CHIPS), pl.ds(first, rows), :]
        target = out.at[:, pl.ds(at, rows), :]
        copies.append(pltpu.make_async_copy(source, target, sems.at[4 + len(copies)]))

    for half, outs in ((1, send), (0, keep)):
        for (_, _, first, rows), out in zip(PARTS, outs):
            for bit in range(2):
                leave(half, bit * HALF + first, rows, out, bit * rows)
        leave(half, BLOCK, TAIL, outs[-1], 0)
    for copy in copies:
        copy.start()
    for copy in copies:
        copy.wait()


def eliminate(members, place, inverse, coupling, rhs, prior, scale, shared, shared_rhs):
    weeks, size, width = coupling.shape
    count = EXTRA + width
    heights = [2 * part[3] for part in PARTS] + [TAIL]
    pieces = [jax.ShapeDtypeStruct((CHIPS, rows, BLOCK), F32) for rows in heights] * 2
    smem = pl.BlockSpec(memory_space=pltpu.SMEM)
    vmem = pl.BlockSpec(memory_space=pltpu.VMEM)
    hbm = pl.BlockSpec(memory_space=pl.ANY)
    scratch = [
        pltpu.VMEM((2 * CHIPS, PIECE, BLOCK), F32),
        pltpu.VMEM((BLOCKS, 8, BLOCK), F32),
        pltpu.VMEM((SUPERS, 8, BLOCK), F32),
        pltpu.SMEM((weeks, TOUCHED), jnp.int32),
        pltpu.SMEM((weeks, TOUCHED), jnp.int32),
        pltpu.SemaphoreType.DMA((4 + 4 * OUTS - 2,)),
    ]
    for _ in range(2):
        scratch += [
            pltpu.VMEM((size, size), F32),
            pltpu.VMEM((size, width), F32),
            pltpu.VMEM((size, width), BF16),
            pltpu.VMEM((size, width), BF16),
            pltpu.VMEM((size, size), BF16),
            pltpu.VMEM((size, size), BF16),
        ] + [pltpu.VMEM((count, size), BF16)] * 4
    return pl.pallas_call(
        eliminate_kernel,
        out_shape=pieces,
        in_specs=[smem, smem, hbm, hbm] + [vmem] * 5,
        out_specs=[hbm] * len(pieces),
        scratch_shapes=scratch,
        compiler_params=pltpu.CompilerParams(vmem_limit_bytes=58 * 1024 * 1024),
        cost_estimate=pl.CostEstimate(
            flops=weeks * 2 * 3 * width * size * (size + 640),
            bytes_accessed=weeks * size * (size + width) * 4,
            transcendentals=0,
        ),
        name="eliminate",
    )(members, place, inverse, coupling, rhs, prior, scale, shared, shared_rhs)


def collect_kernel(spread, piece):
    for axes, crossed, first, rows in PARTS:
        at = slice(first, first + rows)
        for bit in range(2):
            total = None
            for chip in range(CHIPS):
                if chip_bit(axes, crossed, chip) == bit:
                    came = spread[chip, at, :]
                    total = came if total is None else total + came
            piece[bit * HALF + first : bit * HALF + first + rows, :] = total
    total = spread[0, HALF:, :]
    for chip in range(1, CHIPS):
        total = total + spread[chip, HALF:, :]
    piece[BLOCK:, :] = total


def chip_bit(axes, crossed, chip):
    x_hi, z, x_lo, y = chip // 32, chip // 8 % 4, chip // 4 % 2, chip % 4
    at = {"y": y, "z": z}.get(axes[0], 2 * x_hi + x_lo)
    return at // 2 if crossed else at % 2


def collect(spread):
    vmem = pl.BlockSpec(memory_space=pltpu.VMEM)
    return pl.pallas_call(
        collect_kernel,
        out_shape=jax.ShapeDtypeStruct((PIECE, BLOCK), F32),
        in_specs=[vmem],
        out_specs=vmem,
        name="collect",
    )(spread)


def tile_kernel(place, own, other, shared, shared_rhs, prior, scale, matrix, rhs, product, known):
    mine, col = place[1], place[2]
    odd = mine % 2
    half = mine // 2
    upper, lower, level = half < col, half > col, half == col
    first, second = own[:BLOCK, :], other[:BLOCK, :]
    first_turned, second_turned = first.T, second.T
    row = lax.broadcasted_iota(jnp.int32, (BLOCK, BLOCK), 0)
    column = lax.broadcasted_iota(jnp.int32, (BLOCK, BLOCK), 1)
    even_tile = jnp.where(row <= column, first, first_turned)
    odd_tile = jnp.where(
        row > column,
        second,
        jnp.where(row == column, other[BLOCK + 6 : BLOCK + 7, :], second_turned),
    )
    level_even = jnp.logical_and(level, odd == 0)
    level_odd = jnp.logical_and(level, odd == 1)
    turn = jnp.logical_or(lower, level_odd)
    own_tile = jnp.where(level_even, even_tile, jnp.where(turn, first_turned, first))
    other_tile = jnp.where(level_odd, odd_tile, jnp.where(lower, second_turned, second))
    own_left = jnp.logical_or(
        level, jnp.logical_or(jnp.logical_and(upper, odd == 0), jnp.logical_and(lower, odd == 1))
    )
    left = shared[:, :BLOCK] - jnp.where(own_left, own_tile, other_tile)
    right = shared[:, BLOCK:] - jnp.where(own_left, other_tile, own_tile)
    matrix[:, :BLOCK] = left
    matrix[:, BLOCK:] = right
    rhs[...] = shared_rhs[...] - own[BLOCK : BLOCK + 1, :]
    known[...] = prior[pl.ds(mine, 1), :] + scale[...] * own[BLOCK + 1 : BLOCK + 2, :]
    left_known = prior[pl.ds(2 * col, 1), :]
    left_known += own[BLOCK + 3 : BLOCK + 4, :] * own[BLOCK + 2 : BLOCK + 3, :]
    right_known = prior[pl.ds(2 * col + 1, 1), :]
    right_known += own[BLOCK + 5 : BLOCK + 6, :] * own[BLOCK + 4 : BLOCK + 5, :]
    dims = (((1,), (1,)), ((), ()))
    times = functools.partial(
        lax.dot_general,
        dimension_numbers=dims,
        precision=lax.Precision.HIGHEST,
        preferred_element_type=F32,
    )
    left_known = jnp.broadcast_to(left_known, (8, BLOCK))
    right_known = jnp.broadcast_to(right_known, (8, BLOCK))
    product[...] = times(left_known, left) + times(right_known, right)


def own_tile(place, own, other, shared, shared_rhs, prior, scale):
    vmem = pl.BlockSpec(memory_space=pltpu.VMEM)
    line = jax.ShapeDtypeStruct((1, BLOCK), F32)
    return pl.pallas_call(
        tile_kernel,
        out_shape=[
            jax.ShapeDtypeStruct(shared.shape, F32),
            line,
            jax.ShapeDtypeStruct((8, BLOCK), F32),
            line,
        ],
        in_specs=[pl.BlockSpec(memory_space=pltpu.SMEM)] + [vmem] * 6,
        out_specs=[vmem] * 4,
        name="own_tile",
    )(place, own, other, shared, shared_rhs, prior, scale)


def gathered(values):
    copies = jnp.broadcast_to(values[None], (BLOCKS, *values.shape))
    return lax.all_to_all(copies, AXES[:3], 0, 0, tiled=True)


def halved(keep, send):
    came = []
    for part in send:
        came.append(lax.ppermute(part, "core", [(0, 1), (1, 0)]))

    def half(number, bit):
        rows = PARTS[number][3]
        return lax.dynamic_slice_in_dim(
            keep[number], bit * rows, rows, 1
        ) + lax.dynamic_slice_in_dim(came[number], bit * rows, rows, 1)

    bits, got = [], []
    for number, (axes, crossed, _, _) in enumerate(PARTS):
        here = lax.axis_index(axes)
        bits.append(here // 2 if crossed else here % 2)
        pairs = [(i, 3 - i if crossed else i ^ 1) for i in range(4)]
        got.append(lax.ppermute(half(number, 1 - bits[number]), axes, pairs))
    parts = [half(number, bits[number]) + got[number] for number in range(len(PARTS))]
    return jnp.concatenate([*parts, keep[-1] + came[-1]], axis=1)


def swap_pairs():
    pairs = []
    for row in range(BLOCKS):
        for col in range(SUPERS):
            half, odd = row // 2, row % 2
            if half == col:
                to = (row ^ 1, col)
            elif half < col:
                to = (2 * col + odd, half)
            else:
                to = (2 * col + 1 - odd, half)
            pairs.append((row * SUPERS + col, to[0] * SUPERS + to[1]))
    return pairs


def local(
    local_inverse,
    coupling,
    local_rhs,
    members,
    shared_matrix,
    shared_rhs,
    prior_solution,
    preconditioner,
):
    core = lax.axis_index("core")
    row = lax.axis_index(AXES[:3])
    col = lax.axis_index(COL)
    place = jnp.stack([core, row, col]).astype(jnp.int32)
    prior = gathered(prior_solution)
    scale = preconditioner[None]
    pieces = eliminate(
        members,
        place,
        local_inverse,
        coupling,
        local_rhs,
        prior,
        scale,
        shared_matrix,
        shared_rhs[None],
    )
    mixed = halved(pieces[:OUTS], pieces[OUTS:])
    spread = lax.all_to_all(mixed, CHIP_AXES, 0, 0, tiled=True)
    own = collect(spread)
    other = lax.ppermute(own, AXES, swap_pairs())
    matrix, rhs, product, known = own_tile(
        place, own, other, shared_matrix, shared_rhs[None], prior, scale
    )
    products = lax.all_to_all(product, COL, 0, 0, tiled=True)
    rhs = rhs[0]
    solution = known[0] + preconditioner * (rhs - jnp.sum(products, axis=0))
    return (matrix, rhs, solution)


def solution(mesh):
    finer = Mesh(mesh.devices.reshape(2, 4, 2, 2, 4), AXES)
    weeks = P(AXES)
    rows = P(AXES[:3])
    tiles = P(AXES[:3], COL)
    return jax.shard_map(
        local,
        mesh=finer,
        in_specs=(weeks, weeks, weeks, weeks, tiles, rows, rows, rows),
        out_specs=(tiles, rows, rows),
        check_vma=False,
    )
```
